32 devices in a mesh: groups: 2 (over x), row: 16 (over z, y, core).
Axes of the slice: x: 2, y: 2, z: 4, core: 2. Of those that a mesh axis runs over, the one named last changes fastest.
Arguments:
- elevation: float32 [512, 8192], P(('groups', 'row')), parts along dimension 0, may hold values from -2048 to 4096
- bin_index: int32 [512, 8192], P(('groups', 'row')), parts along dimension 0, may hold values from 0 to 1023, as said below
- ranks: int32 [4], P('groups'), parts along dimension 0, may hold values from 20971 to 2076128, as said below
Outputs:
- shaded: float32 [512, 8192], P(('groups', 'row')), parts along dimension 0
The draws below stay inside these ranges and needn't reach their ends.
There are 2 independent parts, one for each index of `groups`. The reference program is written for one: setup_inputs(seed, part) draws one part's arguments, and reference() takes and returns one part's arrays. A program takes and returns all parts, laid end to end along the dimension named above; each array names one. Nothing has to cross between parts.
Inputs may be any that keep to these rules, and one draw needn't show every extreme that they name: The bins have fixed edges: a cell with 0 < bin_index < 1023 has an elevation at or above 2 bin_index and below 2 bin_index + 2; bin 0 holds every elevation below 2 and bin 1024 - 1 every elevation at or above 2046. `ranks`: the first entry lies below 104857 and the second at or above 1992245.
All inputs are finite; a program needn't handle non-finite values.
Results may differ from the reference program's by a relative error of at most 0.0049.
Values sent between devices are 32-bit elements; how exact they have to be, the bound alone decides.
A program may use at most 64 MiB of HBM per device.

```python
import jax
import jax.numpy as jnp
from jax import lax

COLS = 8192
BINS = 1024
NROWS = 256
TOTAL = 2097152


def relief_bins(key):
    subkeys = jax.random.split(key, 6)
    amplitude = jax.random.randint(subkeys[0], (), BINS // 4, BINS * 3 // 4, jnp.int32)
    offset = jax.random.randint(subkeys[1], (), 0, BINS - amplitude - 64, jnp.int32)
    curvature = jax.random.randint(subkeys[2], (), -(BINS // 8), BINS // 8 + 1, jnp.int32)
    column_tilt = jax.random.randint(subkeys[3], (), 0, 48, jnp.int32)
    reversed_trend = jax.random.randint(subkeys[4], (), 0, 2, jnp.int32)
    roughness = jax.random.randint(subkeys[5], (NROWS, COLS), -6, 7, jnp.int32)
    row_fraction = jnp.arange(NROWS, dtype=jnp.int32) * 1024 // NROWS
    row_trend = jnp.where(reversed_trend == 1, 1023 - row_fraction, row_fraction)
    row_term = amplitude * row_trend // 1024 + curvature * row_trend * (1023 - row_trend) // 262144
    column_fraction = jnp.arange(COLS, dtype=jnp.int32) * 1024 // COLS
    column_term = column_tilt * column_fraction // 1024
    field = offset + 32 + row_term[:, None] + column_term[None, :] + roughness
    lowest = jnp.min(field)
    spread = jnp.maximum(jnp.max(field) - lowest, 1)
    scaled = (field - lowest) * (BINS + 76) // spread - 38
    return jnp.clip(scaled, 0, BINS - 1).astype(jnp.int32)


def draw_bin_index(key, part):
    return relief_bins(jax.random.fold_in(key, 7))


def draw_elevation(key, part):
    bin_field = relief_bins(jax.random.fold_in(key, 7))
    offset_key = jax.random.fold_in(key, 8)
    excess_keys = jax.random.split(jax.random.fold_in(key, 9), 3)
    top_extent = jax.random.uniform(excess_keys[0], (), jnp.float32, BINS * 0.5, BINS * 2.0)
    bottom_extent = jax.random.uniform(excess_keys[1], (), jnp.float32, BINS * 0.5, BINS * 2.0)
    unit = jax.random.uniform(excess_keys[2], (NROWS, COLS), jnp.float32, 0.0, 0.999)
    fraction = 0.5 + 0.15 * jax.random.truncated_normal(offset_key, -3.2, 3.2, (NROWS, COLS), jnp.float32)
    profile = unit * unit
    base = 2.0 * (bin_field.astype(jnp.float32) + fraction)
    raised = jnp.where(bin_field == BINS - 1, top_extent * profile, 0.0)
    lowered = jnp.where(bin_field == 0, bottom_extent * profile, 0.0)
    return base + raised - lowered


def draw_ranks(key, part):
    first, second = jax.random.split(key, 2)
    lower = jax.random.randint(first, (1,), TOTAL // 100, TOTAL // 20, jnp.int32)
    upper = jax.random.randint(second, (1,), TOTAL // 100 * 95, TOTAL // 100 * 99, jnp.int32)
    return jnp.concatenate([lower, upper])


def setup_inputs(seed: int = 0, part: int = 0) -> dict:
    splits = jax.random.split(jax.random.key(seed), 4)
    part_splits = jax.random.split(jax.random.fold_in(splits[3], part), 4)
    elevation = draw_elevation(jax.random.fold_in(jax.random.fold_in(splits[3], part), 71), part)
    bin_index = draw_bin_index(jax.random.fold_in(jax.random.fold_in(splits[3], part), 71), part)
    ranks = draw_ranks(jax.random.fold_in(jax.random.fold_in(splits[3], part), 71), part)
    return dict(elevation=elevation, bin_index=bin_index, ranks=ranks)


binomial = (1.0 / 64, 6.0 / 64, 15.0 / 64, 20.0 / 64, 15.0 / 64, 6.0 / 64, 1.0 / 64)
zfactor = 200.0
cos_zenith = 0.70710678
sin_zenith = 0.70710678
light_x = -0.70710678
light_y = 0.70710678

def filter_cols(padded):
    width = padded.shape[1] - 6
    total = binomial[0] * padded[:, 0:width]
    for offset in range(1, 7):
        total = total + binomial[offset] * padded[:, offset:offset + width]
    return total

def filter_rows(padded):
    height = padded.shape[0] - 6
    total = binomial[0] * padded[0:height, :]
    for offset in range(1, 7):
        total = total + binomial[offset] * padded[offset:offset + height, :]
    return total

def shade(smooth, span):
    height = smooth.shape[0] - 2
    width = smooth.shape[1] - 2

    def window(drow, dcol):
        return smooth[drow:drow + height, dcol:dcol + width]
    east = window(0, 2) + 2.0 * window(1, 2) + window(2, 2)
    west = window(0, 0) + 2.0 * window(1, 0) + window(2, 0)
    south = window(2, 0) + 2.0 * window(2, 1) + window(2, 2)
    north = window(0, 0) + 2.0 * window(0, 1) + window(0, 2)
    scale = zfactor / (8.0 * span)
    grad_x = (east - west) * scale
    grad_y = (south - north) * scale
    light = (cos_zenith - sin_zenith * (light_x * grad_x + light_y * grad_y)) * lax.rsqrt(1.0 + grad_x * grad_x + grad_y * grad_y)
    return jnp.maximum(light, 0.0)

def reference(elevation, bin_index, ranks):
    counts = jnp.zeros((BINS,), jnp.float32).at[bin_index.reshape(-1)].add(1.0)
    span = jnp.max(elevation) - jnp.min(elevation)
    cumulative = jnp.cumsum(counts.astype(jnp.int32), dtype=jnp.int32)
    table = jnp.clip((cumulative - ranks[0]).astype(jnp.float32) / (ranks[1] - ranks[0]).astype(jnp.float32), 0.0, 1.0).astype(jnp.bfloat16)
    stretch = table.astype(jnp.float32)[bin_index]
    padded = jnp.pad(elevation, 4)
    smooth = filter_rows(filter_cols(padded))
    light = shade(smooth, span)
    return stretch * (0.5 + light)
```

```python
import functools

import jax
import jax.numpy as jnp
from jax import lax
from jax.experimental import pallas as pl
from jax.experimental.pallas import tpu as pltpu
from jax.sharding import PartitionSpec as P

BINS = 1024
zfactor = 200.0
cos_zenith = 0.70710678
sin_zenith = 0.70710678
light_x = -0.70710678
light_y = 0.70710678
LANES = 128
HALO = 4
PAD = 128
SMOOTH = (1.0, 8.0, 28.0, 56.0, 70.0, 56.0, 28.0, 8.0, 1.0)
SLOPE = (-1.0, -6.0, -14.0, -14.0, 0.0, 14.0, 14.0, 6.0, 1.0)
UPPER = 16
LOWER = BINS // UPPER


def bins_of(cells):
    return jnp.floor(jnp.clip(cells * 0.5, 0.0, float(BINS - 1)))


def row_weights(weights, height):
    depth = 3 * (height + 8) + 8
    row = lax.broadcasted_iota(jnp.int32, (height, depth), 0)
    col = lax.broadcasted_iota(jnp.int32, (height, depth), 1)
    own = lax.rem(col, height)
    edge = lax.rem(jnp.maximum(col - 3 * height, 0), 8)
    edge = jnp.where(edge < HALO, height + edge, edge - 8)
    source = jnp.where(col < 3 * height, own, edge)
    source = jnp.where(col < 3 * (height + 8), source, 4 * height)
    delta = source - row
    out = jnp.zeros((height, depth), jnp.float32)
    for k, weight in enumerate(weights):
        out = jnp.where(delta == k - HALO, weight, out)
    return out.astype(jnp.bfloat16)


def split3(cells):
    first = cells.astype(jnp.bfloat16).astype(jnp.float32)
    rest = cells - first
    second = rest.astype(jnp.bfloat16).astype(jnp.float32)
    return first, second, rest - second


def stacked(cells):
    halo = split3(cells[0:8])
    own = split3(cells[8:])
    return jnp.concatenate([*own, *halo, jnp.zeros_like(halo[0])], axis=0).astype(jnp.bfloat16)


def kernel(n, chunk, ranks_ref, elev_ref, out_ref, cells, upper, lower, send, recv, slope_x, slope_y,
           result, in_sem, halo_send, halo_recv, send_sem, recv_sem, out_sem):
    me = lax.axis_index("row")
    height, width = elev_ref.shape
    chunks = width // chunk
    inner = pl.ds(PAD, width)

    load = pltpu.make_async_copy(elev_ref, cells.at[pl.ds(8, height), inner], in_sem)
    load.start()

    barrier = pltpu.get_barrier_semaphore()

    def greet(k, carry):
        pl.semaphore_signal(barrier, inc=1, device_id={"row": lax.rem(me + k, n)},
                            device_id_type=pl.DeviceIdType.MESH)
        return carry

    lax.fori_loop(1, n, greet, 0)

    zeros = jnp.zeros((height + 8, PAD), jnp.float32)
    cells[:, pl.ds(0, PAD)] = zeros
    cells[:, pl.ds(PAD + width, PAD)] = zeros

    @pl.when(me == 0)
    def _():
        cells[4:8, inner] = jnp.zeros((4, width), jnp.float32)

    @pl.when(me == n - 1)
    def _():
        cells[0:4, inner] = jnp.zeros((4, width), jnp.float32)

    load.wait()
    pl.semaphore_wait(barrier, n - 1)

    down = pltpu.make_async_remote_copy(
        src_ref=cells.at[pl.ds(8 + height - HALO, HALO), inner], dst_ref=cells.at[pl.ds(4, HALO), inner],
        send_sem=halo_send.at[0], recv_sem=halo_recv.at[0],
        device_id={"row": lax.rem(me + 1, n)}, device_id_type=pl.DeviceIdType.MESH)
    up = pltpu.make_async_remote_copy(
        src_ref=cells.at[pl.ds(8, HALO), inner], dst_ref=cells.at[pl.ds(0, HALO), inner],
        send_sem=halo_send.at[1], recv_sem=halo_recv.at[1],
        device_id={"row": lax.rem(me + n - 1, n)}, device_id_type=pl.DeviceIdType.MESH)

    @pl.when(me < n - 1)
    def _():
        down.start()

    @pl.when(me > 0)
    def _():
        up.start()

    def prepare(i, carry):
        top, bottom = carry
        at = pl.multiple_of(i * chunk, chunk)
        block = cells[pl.ds(8, height), pl.ds(at + PAD, chunk)]
        bins = bins_of(block)
        high = jnp.floor(bins * (1.0 / LOWER))
        upper[:, pl.ds(at, chunk)] = high
        lower[:, pl.ds(at, chunk)] = bins - high * LOWER
        for r in range(height // 8):
            for c in range(chunk // LANES):
                piece = block[8 * r : 8 * r + 8, c * LANES : (c + 1) * LANES]
                top, bottom = jnp.maximum(top, piece), jnp.minimum(bottom, piece)
        return top, bottom

    start = cells[8:16, PAD : PAD + LANES]
    top, bottom = lax.fori_loop(0, chunks, prepare, (start, start))

    urow = lax.broadcasted_iota(jnp.int32, (UPPER, chunk), 0)
    upper_iota = (2 * lax.rem(urow, 8) + urow // 8).astype(jnp.float32).astype(jnp.bfloat16)
    lower_iota = lax.broadcasted_iota(jnp.int32, (LOWER, chunk), 0).astype(jnp.float32).astype(jnp.bfloat16)

    def count(i, total):
        at = pl.multiple_of(i * chunk, chunk)
        for r in range(height):
            high = jnp.broadcast_to(upper[r : r + 1, pl.ds(at, chunk)], (UPPER, chunk)).astype(jnp.bfloat16)
            low = jnp.broadcast_to(lower[r : r + 1, pl.ds(at, chunk)], (LOWER, chunk)).astype(jnp.bfloat16)
            one, zero = jnp.ones((), jnp.bfloat16), jnp.zeros((), jnp.bfloat16)
            hot_u = jnp.where(high == upper_iota, one, zero)
            hot_l = jnp.where(low == lower_iota, one, zero)
            total = total + lax.dot_general(hot_u, hot_l, (((1,), (1,)), ((), ())),
                                            preferred_element_type=jnp.float32)
        return total

    total = lax.fori_loop(0, chunks, count, jnp.zeros((UPPER, LOWER), jnp.float32))
    counts = jnp.concatenate([total[0:8], total[8:16]], axis=1)
    send[0:8, :] = counts
    send[8:9, :] = jnp.max(top, axis=0, keepdims=True)
    send[9:10, :] = jnp.max(-bottom, axis=0, keepdims=True)

    def copy_to(k):
        return pltpu.make_async_remote_copy(
            src_ref=send, dst_ref=recv.at[k], send_sem=send_sem.at[k], recv_sem=recv_sem.at[k],
            device_id={"row": lax.rem(me + k, n)}, device_id_type=pl.DeviceIdType.MESH)

    def post(k, carry):
        copy_to(k).start()
        return carry

    lax.fori_loop(1, n, post, 0)

    @pl.when(me > 0)
    def _():
        down.wait_recv()

    @pl.when(me < n - 1)
    def _():
        up.wait_recv()

    smooth_w = row_weights(SMOOTH, height)
    slope_w = row_weights(SLOPE, height)
    span_w = chunk + 2 * PAD

    def stencil(i, carry):
        at = pl.multiple_of(i * chunk, chunk)
        x = cells[:, pl.ds(at, span_w)]
        for k in range(7):
            x = x + pltpu.roll(x, 1 if k % 2 else span_w - 1, 1)
        moved = pltpu.roll(x, 1, 1)
        rise = (x - moved)[:, PAD : PAD + chunk]
        level = (x + moved)[:, PAD : PAD + chunk]
        slope_x[:, pl.ds(at, chunk)] = jnp.dot(smooth_w, stacked(rise), preferred_element_type=jnp.float32)
        slope_y[:, pl.ds(at, chunk)] = jnp.dot(slope_w, stacked(level), preferred_element_type=jnp.float32)
        return carry

    lax.fori_loop(0, chunks, stencil, 0)

    def take(k, carry):
        copy_to(k).wait_recv()
        got = recv[k]
        return carry[0] + got[0:8], jnp.maximum(carry[1], got[8:10])

    counts, ends = lax.fori_loop(1, n, take, (send[0:8, :], send[8:10, :]))
    ends = jnp.max(ends, axis=1, keepdims=True)
    span = ends[0:1] + ends[1:2]
    scale = jnp.broadcast_to(zfactor / (8.0 * span) * (1.0 / 4096.0), (8, LANES))

    whole = counts.astype(jnp.int32)
    lane_in = lax.broadcasted_iota(jnp.int32, (LANES, LANES), 0)
    lane_out = lax.broadcasted_iota(jnp.int32, (LANES, LANES), 1)
    triangle = jnp.where(lane_in <= lane_out, 1.0, 0.0).astype(jnp.bfloat16)
    digits = jnp.concatenate([(whole & 255), ((whole >> 8) & 255), (whole >> 16), jnp.zeros_like(whole)],
                             axis=0).astype(jnp.float32).astype(jnp.bfloat16)
    sums = jnp.dot(digits, triangle, preferred_element_type=jnp.float32)
    within = sums[0:8] + 256.0 * sums[8:16] + 65536.0 * sums[16:24]
    before = jnp.zeros((1, 1), jnp.float32)
    rows = []
    first, second = ranks_ref[0], ranks_ref[1]
    for b in range(8):
        rows.append(before)
        before = before + within[b : b + 1, LANES - 1 : LANES]
    offsets = jnp.concatenate(rows, axis=0)
    cumulative = (within + offsets).astype(jnp.int32)
    divisor = jnp.full((8, LANES), second - first, jnp.int32).astype(jnp.float32)
    table = jnp.clip((cumulative - first).astype(jnp.float32) / divisor, 0.0, 1.0)
    table = table.astype(jnp.bfloat16).astype(jnp.float32)
    tables = [jnp.broadcast_to(table[b : b + 1], (8, LANES)) for b in range(8)]

    def out_copy(i):
        at = pl.multiple_of(i * chunk, chunk)
        where = (slice(None), pl.ds(at, chunk))
        return pltpu.make_async_copy(result.at[where], out_ref.at[where], out_sem.at[i])

    def finish(i, carry):
        at = pl.multiple_of(i * chunk, chunk)
        for r in range(height // 8):
            for c in range(chunk // LANES):
                rows = pl.ds(8 * r, 8)
                cols = pl.ds(at + c * LANES, LANES)
                index = bins_of(cells[pl.ds(8 + 8 * r, 8), pl.ds(at + PAD + c * LANES, LANES)]).astype(jnp.int32)
                group, lane = index >> 7, index & 127
                stretch = jnp.take_along_axis(tables[0], lane, axis=1)
                for b in range(1, 8):
                    stretch = jnp.where(group == b, jnp.take_along_axis(tables[b], lane, axis=1), stretch)
                gx = slope_x[rows, cols] * scale
                gy = slope_y[rows, cols] * scale
                light = (cos_zenith - sin_zenith * (light_x * gx + light_y * gy)) * lax.rsqrt(
                    1.0 + gx * gx + gy * gy)
                result[rows, cols] = stretch * (0.5 + jnp.maximum(light, 0.0))
        out_copy(i).start()
        return carry

    lax.fori_loop(0, chunks, finish, 0)

    @pl.when(me < n - 1)
    def _():
        down.wait_send()

    @pl.when(me > 0)
    def _():
        up.wait_send()

    def drain(k, carry):
        copy_to(k).wait_send()
        return carry

    lax.fori_loop(1, n, drain, 0)

    def flush(i, carry):
        out_copy(i).wait()
        return carry

    lax.fori_loop(0, chunks, flush, 0)


def chunk_of(width):
    chunk = 1024
    while width % chunk:
        chunk //= 2
    return chunk


def solution(mesh):
    n = mesh.shape["row"]

    def body(elevation, bin_index, ranks):
        height, width = elevation.shape
        chunk = chunk_of(width)
        grid = (height, width)
        return pl.pallas_call(
            functools.partial(kernel, n, chunk),
            out_shape=jax.ShapeDtypeStruct(grid, jnp.float32),
            in_specs=[pl.BlockSpec(memory_space=pltpu.SMEM), pl.BlockSpec(memory_space=pl.ANY)],
            out_specs=pl.BlockSpec(memory_space=pl.ANY),
            scratch_shapes=[
                pltpu.VMEM((height + 8, width + 2 * PAD), jnp.float32),
                pltpu.VMEM(grid, jnp.float32),
                pltpu.VMEM(grid, jnp.float32),
                pltpu.VMEM((10, LANES), jnp.float32),
                pltpu.VMEM((n, 10, LANES), jnp.float32),
                pltpu.VMEM(grid, jnp.float32),
                pltpu.VMEM(grid, jnp.float32),
                pltpu.VMEM(grid, jnp.float32),
                pltpu.SemaphoreType.DMA,
                pltpu.SemaphoreType.DMA((2,)),
                pltpu.SemaphoreType.DMA((2,)),
                pltpu.SemaphoreType.DMA((n,)),
                pltpu.SemaphoreType.DMA((n,)),
                pltpu.SemaphoreType.DMA((width // chunk,)),
            ],
            compiler_params=pltpu.CompilerParams(collective_id=0, has_side_effects=True),
        )(ranks, elevation)

    in_specs = (P(("groups", "row"), None), P(("groups", "row"), None), P("groups"))
    return jax.shard_map(body, mesh=mesh, in_specs=in_specs, out_specs=P(("groups", "row"), None), check_vma=False)
```

```python
import functools

import jax
import jax.numpy as jnp
from jax import lax
from jax.experimental import pallas as pl
from jax.experimental.pallas import tpu as pltpu
from jax.sharding import PartitionSpec as P

BINS = 1024
zfactor = 200.0
cos_zenith = 0.70710678
sin_zenith = 0.70710678
light_x = -0.70710678
light_y = 0.70710678
LANES = 128
HALO = 4
PAD = 128
SMOOTH = (1.0, 8.0, 28.0, 56.0, 70.0, 56.0, 28.0, 8.0, 1.0)
SLOPE = (-1.0, -6.0, -14.0, -14.0, 0.0, 14.0, 14.0, 6.0, 1.0)
UPPER = 32
LOWER = BINS // UPPER


def bins_of(cells):
    return jnp.floor(jnp.clip(cells * 0.5, 0.0, float(BINS - 1)))


def row_weights(weights, height, halo):
    rows = 8 if halo else height
    row = lax.broadcasted_iota(jnp.int32, (height, 4 * rows if halo else 3 * rows), 0)
    col = lax.broadcasted_iota(jnp.int32, row.shape, 1)
    source = lax.rem(col, rows)
    if halo:
        source = jnp.where(source < HALO, height + source, source - 8)
        source = jnp.where(col < 3 * rows, source, 4 * height)
    delta = source - row
    out = jnp.zeros(row.shape, jnp.float32)
    for k, weight in enumerate(weights):
        out = jnp.where(delta == k - HALO, weight, out)
    return out.astype(jnp.bfloat16)


def stacked(cells):
    first = cells.astype(jnp.bfloat16).astype(jnp.float32)
    rest = cells - first
    second = rest.astype(jnp.bfloat16).astype(jnp.float32)
    parts = [first, second, rest - second]
    if cells.shape[0] == 8:
        parts.append(jnp.zeros_like(first))
    return jnp.concatenate(parts, axis=0).astype(jnp.bfloat16)


def columns(x):
    wide = x.shape[1]
    for k in range(7):
        x = x + pltpu.roll(x, 1 if k % 2 else wide - 1, 1)
    moved = pltpu.roll(x, 1, 1)
    inside = slice(PAD, wide - PAD)
    return (x - moved)[:, inside], (x + moved)[:, inside]


def kernel(n, chunk, elev_ref, out_ref, slope_x, slope_y, cells, upper, lower, send, recv, in_sem, halo_send, halo_recv, send_sem, recv_sem):
    me = lax.axis_index("row")
    height, width = elev_ref.shape
    chunks = width // chunk
    inner = pl.ds(PAD, width)

    load = pltpu.make_async_copy(elev_ref, cells.at[pl.ds(8, height), inner], in_sem)
    load.start()

    barrier = pltpu.get_barrier_semaphore()

    def greet(k, carry):
        pl.semaphore_signal(barrier, inc=1, device_id={"row": lax.rem(me + k, n)},
                            device_id_type=pl.DeviceIdType.MESH)
        return carry

    lax.fori_loop(1, n, greet, 0)

    zeros = jnp.zeros((height + 8, PAD), jnp.float32)
    cells[:, pl.ds(0, PAD)] = zeros
    cells[:, pl.ds(PAD + width, PAD)] = zeros

    @pl.when(me == 0)
    def _():
        cells[4:8, inner] = jnp.zeros((4, width), jnp.float32)

    @pl.when(me == n - 1)
    def _():
        cells[0:4, inner] = jnp.zeros((4, width), jnp.float32)

    load.wait()

    down = pltpu.make_async_remote_copy(
        src_ref=cells.at[pl.ds(8 + height - HALO, HALO), inner], dst_ref=cells.at[pl.ds(4, HALO), inner],
        send_sem=halo_send.at[0], recv_sem=halo_recv.at[0],
        device_id={"row": lax.rem(me + 1, n)}, device_id_type=pl.DeviceIdType.MESH)
    up = pltpu.make_async_remote_copy(
        src_ref=cells.at[pl.ds(8, HALO), inner], dst_ref=cells.at[pl.ds(0, HALO), inner],
        send_sem=halo_send.at[1], recv_sem=halo_recv.at[1],
        device_id={"row": lax.rem(me + n - 1, n)}, device_id_type=pl.DeviceIdType.MESH)

    def prepare(i, carry):
        top, bottom = carry
        at = pl.multiple_of(i * chunk, chunk)
        block = cells[pl.ds(8, height), pl.ds(at + PAD, chunk)]
        bins = bins_of(block)
        high = jnp.floor(bins * (1.0 / LOWER))
        upper[:, pl.ds(at, chunk)] = high
        lower[:, pl.ds(at, chunk)] = bins - high * LOWER
        for r in range(height // 8):
            for c in range(chunk // LANES):
                piece = block[8 * r : 8 * r + 8, c * LANES : (c + 1) * LANES]
                top, bottom = jnp.maximum(top, piece), jnp.minimum(bottom, piece)
        return top, bottom

    start = cells[8:16, PAD : PAD + LANES]
    top, bottom = lax.fori_loop(0, chunks, prepare, (start, start))

    urow = lax.broadcasted_iota(jnp.int32, (UPPER, chunk), 0)
    upper_iota = (4 * lax.rem(urow, 8) + urow // 8).astype(jnp.float32).astype(jnp.bfloat16)
    lower_iota = lax.broadcasted_iota(jnp.int32, (LOWER, chunk), 0).astype(jnp.float32).astype(jnp.bfloat16)

    def count(i, total):
        at = pl.multiple_of(i * chunk, chunk)
        for r in range(height):
            high = jnp.broadcast_to(upper[r : r + 1, pl.ds(at, chunk)], (UPPER, chunk)).astype(jnp.bfloat16)
            low = jnp.broadcast_to(lower[r : r + 1, pl.ds(at, chunk)], (LOWER, chunk)).astype(jnp.bfloat16)
            one, zero = jnp.ones((), jnp.bfloat16), jnp.zeros((), jnp.bfloat16)
            hot_u = jnp.where(high == upper_iota, one, zero)
            hot_l = jnp.where(low == lower_iota, one, zero)
            total = total + lax.dot_general(hot_u, hot_l, (((1,), (1,)), ((), ())),
                                            preferred_element_type=jnp.float32)
        return total

    total = lax.fori_loop(0, chunks, count, jnp.zeros((UPPER, LOWER), jnp.float32))
    counts = jnp.concatenate([total[8 * q : 8 * q + 8] for q in range(UPPER // 8)], axis=1)
    send[0:8, :] = counts
    send[8:9, :] = jnp.max(top, axis=0, keepdims=True)
    send[9:10, :] = jnp.max(-bottom, axis=0, keepdims=True)

    def copy_to(k):
        return pltpu.make_async_remote_copy(
            src_ref=send, dst_ref=recv.at[k], send_sem=send_sem.at[k], recv_sem=recv_sem.at[k],
            device_id={"row": lax.rem(me + k, n)}, device_id_type=pl.DeviceIdType.MESH)

    def post(k, carry):
        copy_to(k).start()
        return carry

    pl.semaphore_wait(barrier, n - 1)
    lax.fori_loop(1, n, post, 0)

    @pl.when(me < n - 1)
    def _():
        down.start()

    @pl.when(me > 0)
    def _():
        up.start()


    own_smooth, own_slope = row_weights(SMOOTH, height, False), row_weights(SLOPE, height, False)

    def own_rows(i, carry):
        at = pl.multiple_of(i * chunk, chunk)
        rise, level = columns(cells[pl.ds(8, height), pl.ds(at, chunk + 2 * PAD)])
        slope_x[:, pl.ds(at, chunk)] = jnp.dot(own_smooth, stacked(rise), preferred_element_type=jnp.float32)
        slope_y[:, pl.ds(at, chunk)] = jnp.dot(own_slope, stacked(level), preferred_element_type=jnp.float32)
        return carry

    lax.fori_loop(0, chunks, own_rows, 0, unroll=2)

    @pl.when(me > 0)
    def _():
        down.wait_recv()

    @pl.when(me < n - 1)
    def _():
        up.wait_recv()

    halo_smooth, halo_slope = row_weights(SMOOTH, height, True), row_weights(SLOPE, height, True)

    def halo_rows(i, carry):
        at = pl.multiple_of(i * chunk, chunk)
        rise, level = columns(cells[pl.ds(0, 8), pl.ds(at, chunk + 2 * PAD)])
        slope_x[:, pl.ds(at, chunk)] += jnp.dot(halo_smooth, stacked(rise), preferred_element_type=jnp.float32)
        slope_y[:, pl.ds(at, chunk)] += jnp.dot(halo_slope, stacked(level), preferred_element_type=jnp.float32)
        return carry

    lax.fori_loop(0, chunks, halo_rows, 0, unroll=True)

    def take(k, carry):
        copy_to(k).wait_recv()
        got = recv[k]
        return carry[0] + got[0:8], jnp.maximum(carry[1], got[8:10])

    counts, ends = lax.fori_loop(1, n, take, (send[0:8, :], send[8:10, :]))
    out_ref[0:8, :] = counts
    out_ref[8:10, :] = ends

    @pl.when(me < n - 1)
    def _():
        down.wait_send()

    @pl.when(me > 0)
    def _():
        up.wait_send()

    def drain(k, carry):
        copy_to(k).wait_send()
        return carry

    lax.fori_loop(1, n, drain, 0)


def shade_kernel(chunk, ranks_ref, sums_ref, cells, slope_x, slope_y, out_ref, result, out_sem):
    height, width = cells.shape
    chunks = width // chunk
    counts = sums_ref[0:8, :]
    ends = jnp.max(sums_ref[8:10, :], axis=1, keepdims=True)
    span = ends[0:1] + ends[1:2]
    scale = jnp.broadcast_to(zfactor / (8.0 * span) * (1.0 / 4096.0), (8, LANES))

    whole = counts.astype(jnp.int32)
    lane_in = lax.broadcasted_iota(jnp.int32, (LANES, LANES), 0)
    lane_out = lax.broadcasted_iota(jnp.int32, (LANES, LANES), 1)
    triangle = jnp.where(lane_in <= lane_out, 1.0, 0.0).astype(jnp.bfloat16)
    digits = jnp.concatenate([(whole & 255), ((whole >> 8) & 255), (whole >> 16), jnp.zeros_like(whole)],
                             axis=0).astype(jnp.float32).astype(jnp.bfloat16)
    sums = jnp.dot(digits, triangle, preferred_element_type=jnp.float32)
    within = sums[0:8] + 256.0 * sums[8:16] + 65536.0 * sums[16:24]
    before = jnp.zeros((1, 1), jnp.float32)
    rows = []
    first, second = ranks_ref[0], ranks_ref[1]
    for b in range(8):
        rows.append(before)
        before = before + within[b : b + 1, LANES - 1 : LANES]
    offsets = jnp.concatenate(rows, axis=0)
    cumulative = (within + offsets).astype(jnp.int32)
    divisor = jnp.full((8, LANES), second - first, jnp.int32).astype(jnp.float32)
    table = jnp.clip((cumulative - first).astype(jnp.float32) / divisor, 0.0, 1.0)
    table = table.astype(jnp.bfloat16).astype(jnp.float32)
    tables = [jnp.broadcast_to(table[b : b + 1], (8, LANES)) for b in range(8)]

    def out_copy(i):
        at = pl.multiple_of(i * chunk, chunk)
        where = (slice(None), pl.ds(at, chunk))
        return pltpu.make_async_copy(result.at[where], out_ref.at[where], out_sem.at[i])

    def finish(i, carry):
        at = pl.multiple_of(i * chunk, chunk)
        for r in range(height // 8):
            for c in range(chunk // LANES):
                rows = pl.ds(8 * r, 8)
                cols = pl.ds(at + c * LANES, LANES)
                index = bins_of(cells[rows, cols]).astype(jnp.int32)
                group, lane = index >> 7, index & 127
                stretch = jnp.take_along_axis(tables[0], lane, axis=1)
                for b in range(1, 8):
                    stretch = jnp.where(group == b, jnp.take_along_axis(tables[b], lane, axis=1), stretch)
                gx = slope_x[rows, cols] * scale
                gy = slope_y[rows, cols] * scale
                light = (cos_zenith - sin_zenith * (light_x * gx + light_y * gy)) * lax.rsqrt(
                    1.0 + gx * gx + gy * gy)
                result[rows, cols] = stretch * (0.5 + jnp.maximum(light, 0.0))
        out_copy(i).start()
        return carry

    lax.fori_loop(0, chunks, finish, 0)

    def flush(i, carry):
        out_copy(i).wait()
        return carry

    lax.fori_loop(0, chunks, flush, 0)


def chunk_of(width):
    chunk = 1024
    while width % chunk:
        chunk //= 2
    return chunk


def solution(mesh):
    n = mesh.shape["row"]

    def body(elevation, bin_index, ranks):
        height, width = elevation.shape
        chunk = chunk_of(width)
        chunks = width // chunk
        grid = (height, width)
        room = 32 * height * width * 4
        block = pltpu.VMEM(grid, jnp.float32)
        whole = jax.ShapeDtypeStruct(grid, jnp.float32)
        anywhere = pl.BlockSpec(memory_space=pl.ANY)
        inside = pl.BlockSpec(memory_space=pltpu.VMEM)
        sums, slope_x, slope_y = pl.pallas_call(
            functools.partial(kernel, n, chunk),
            out_shape=[jax.ShapeDtypeStruct((10, LANES), jnp.float32), whole, whole],
            in_specs=[anywhere],
            out_specs=[inside, inside, inside],
            scratch_shapes=[
                pltpu.VMEM((height + 8, width + 2 * PAD), jnp.float32),
                block,
                block,
                pltpu.VMEM((10, LANES), jnp.float32),
                pltpu.VMEM((n, 10, LANES), jnp.float32),
                pltpu.SemaphoreType.DMA,
                pltpu.SemaphoreType.DMA((2,)),
                pltpu.SemaphoreType.DMA((2,)),
                pltpu.SemaphoreType.DMA((n,)),
                pltpu.SemaphoreType.DMA((n,)),
            ],
            compiler_params=pltpu.CompilerParams(collective_id=0, has_side_effects=True, vmem_limit_bytes=room),
        )(elevation)
        return pl.pallas_call(
            functools.partial(shade_kernel, chunk),
            out_shape=whole,
            in_specs=[pl.BlockSpec(memory_space=pltpu.SMEM), inside, inside, inside, inside],
            out_specs=anywhere,
            scratch_shapes=[block, pltpu.SemaphoreType.DMA((chunks,))],
            compiler_params=pltpu.CompilerParams(vmem_limit_bytes=room),
        )(ranks, sums, elevation, slope_x, slope_y)

    in_specs = (P(("groups", "row"), None), P(("groups", "row"), None), P("groups"))
    return jax.shard_map(body, mesh=mesh, in_specs=in_specs, out_specs=P(("groups", "row"), None), check_vma=False)
```

```python
import functools

import jax
import jax.numpy as jnp
from jax import lax
from jax.experimental import pallas as pl
from jax.experimental.pallas import tpu as pltpu
from jax.sharding import PartitionSpec as P

BINS = 1024
zfactor = 200.0
cos_zenith = 0.70710678
sin_zenith = 0.70710678
light_x = -0.70710678
light_y = 0.70710678
LANES = 128
HALO = 4
PAD = 128
SMOOTH = (1.0, 8.0, 28.0, 56.0, 70.0, 56.0, 28.0, 8.0, 1.0)
SLOPE = (-1.0, -6.0, -14.0, -14.0, 0.0, 14.0, 14.0, 6.0, 1.0)
UPPER = 32
LOWER = BINS // UPPER


def bins_of(cells):
    return jnp.floor(jnp.clip(cells * 0.5, 0.0, float(BINS - 1)))


def row_weights(weights, height, halo):
    rows = 8 if halo else height
    row = lax.broadcasted_iota(jnp.int32, (height, 4 * rows if halo else 3 * rows), 0)
    col = lax.broadcasted_iota(jnp.int32, row.shape, 1)
    source = lax.rem(col, rows)
    if halo:
        source = jnp.where(source < HALO, height + source, source - 8)
        source = jnp.where(col < 3 * rows, source, 4 * height)
    delta = source - row
    out = jnp.zeros(row.shape, jnp.float32)
    for k, weight in enumerate(weights):
        out = jnp.where(delta == k - HALO, weight, out)
    return out.astype(jnp.bfloat16)


def stacked(cells):
    first = cells.astype(jnp.bfloat16).astype(jnp.float32)
    rest = cells - first
    second = rest.astype(jnp.bfloat16).astype(jnp.float32)
    parts = [first, second, rest - second]
    if cells.shape[0] == 8:
        parts.append(jnp.zeros_like(first))
    return jnp.concatenate(parts, axis=0).astype(jnp.bfloat16)


def columns(x):
    wide = x.shape[1]
    for k in range(7):
        x = x + pltpu.roll(x, 1 if k % 2 else wide - 1, 1)
    moved = pltpu.roll(x, 1, 1)
    inside = slice(PAD, wide - PAD)
    return (x - moved)[:, inside], (x + moved)[:, inside]


def kernel(n, chunk, ranks_ref, elev_ref, out_ref, index, slope_x, slope_y, cells, upper, lower, send, recv, ranks, in_sem, rank_sem, halo_send, halo_recv, send_sem, recv_sem):
    me = lax.axis_index("row")
    height, width = elev_ref.shape
    chunks = width // chunk
    inner = pl.ds(PAD, width)

    load = pltpu.make_async_copy(elev_ref, cells.at[pl.ds(8, height), inner], in_sem)
    load.start()
    rank_load = pltpu.make_async_copy(ranks_ref, ranks, rank_sem)
    rank_load.start()

    barrier = pltpu.get_barrier_semaphore()

    def greet(k, carry):
        pl.semaphore_signal(barrier, inc=1, device_id={"row": lax.rem(me + k, n)},
                            device_id_type=pl.DeviceIdType.MESH)
        return carry

    lax.fori_loop(1, n, greet, 0)

    zeros = jnp.zeros((height + 8, PAD), jnp.float32)
    cells[:, pl.ds(0, PAD)] = zeros
    cells[:, pl.ds(PAD + width, PAD)] = zeros

    @pl.when(me == 0)
    def _():
        cells[4:8, inner] = jnp.zeros((4, width), jnp.float32)

    @pl.when(me == n - 1)
    def _():
        cells[0:4, inner] = jnp.zeros((4, width), jnp.float32)

    load.wait()

    down = pltpu.make_async_remote_copy(
        src_ref=cells.at[pl.ds(8 + height - HALO, HALO), inner], dst_ref=cells.at[pl.ds(4, HALO), inner],
        send_sem=halo_send.at[0], recv_sem=halo_recv.at[0],
        device_id={"row": lax.rem(me + 1, n)}, device_id_type=pl.DeviceIdType.MESH)
    up = pltpu.make_async_remote_copy(
        src_ref=cells.at[pl.ds(8, HALO), inner], dst_ref=cells.at[pl.ds(0, HALO), inner],
        send_sem=halo_send.at[1], recv_sem=halo_recv.at[1],
        device_id={"row": lax.rem(me + n - 1, n)}, device_id_type=pl.DeviceIdType.MESH)

    def prepare(i, carry):
        top, bottom = carry
        at = pl.multiple_of(i * chunk, chunk)
        block = cells[pl.ds(8, height), pl.ds(at + PAD, chunk)]
        bins = bins_of(block)
        index[:, pl.ds(at, chunk)] = bins.astype(jnp.int32)
        high = jnp.floor(bins * (1.0 / LOWER))
        upper[:, pl.ds(at, chunk)] = high
        lower[:, pl.ds(at, chunk)] = bins - high * LOWER
        for r in range(height // 8):
            for c in range(chunk // LANES):
                piece = block[8 * r : 8 * r + 8, c * LANES : (c + 1) * LANES]
                top, bottom = jnp.maximum(top, piece), jnp.minimum(bottom, piece)
        return top, bottom

    start = cells[8:16, PAD : PAD + LANES]
    top, bottom = lax.fori_loop(0, chunks, prepare, (start, start))

    urow = lax.broadcasted_iota(jnp.int32, (UPPER, chunk), 0)
    upper_iota = (4 * lax.rem(urow, 8) + urow // 8).astype(jnp.float32).astype(jnp.bfloat16)
    lower_iota = lax.broadcasted_iota(jnp.int32, (LOWER, chunk), 0).astype(jnp.float32).astype(jnp.bfloat16)

    def count(i, total):
        at = pl.multiple_of(i * chunk, chunk)
        for r in range(height):
            high = jnp.broadcast_to(upper[r : r + 1, pl.ds(at, chunk)], (UPPER, chunk)).astype(jnp.bfloat16)
            low = jnp.broadcast_to(lower[r : r + 1, pl.ds(at, chunk)], (LOWER, chunk)).astype(jnp.bfloat16)
            one, zero = jnp.ones((), jnp.bfloat16), jnp.zeros((), jnp.bfloat16)
            hot_u = jnp.where(high == upper_iota, one, zero)
            hot_l = jnp.where(low == lower_iota, one, zero)
            total = total + lax.dot_general(hot_u, hot_l, (((1,), (1,)), ((), ())),
                                            preferred_element_type=jnp.float32)
        return total

    total = lax.fori_loop(0, chunks, count, jnp.zeros((UPPER, LOWER), jnp.float32))
    counts = jnp.concatenate([total[8 * q : 8 * q + 8] for q in range(UPPER // 8)], axis=1)
    send[0:8, :] = counts
    send[8:9, :] = jnp.max(top, axis=0, keepdims=True)
    send[9:10, :] = jnp.max(-bottom, axis=0, keepdims=True)

    def copy_to(k):
        return pltpu.make_async_remote_copy(
            src_ref=send, dst_ref=recv.at[k], send_sem=send_sem.at[k], recv_sem=recv_sem.at[k],
            device_id={"row": lax.rem(me + k, n)}, device_id_type=pl.DeviceIdType.MESH)

    def post(k, carry):
        copy_to(k).start()
        return carry

    pl.semaphore_wait(barrier, n - 1)
    lax.fori_loop(1, n, post, 0)

    @pl.when(me < n - 1)
    def _():
        down.start()

    @pl.when(me > 0)
    def _():
        up.start()


    own_smooth, own_slope = row_weights(SMOOTH, height, False), row_weights(SLOPE, height, False)

    def own_rows(i, carry):
        at = pl.multiple_of(i * chunk, chunk)
        rise, level = columns(cells[pl.ds(8, height), pl.ds(at, chunk + 2 * PAD)])
        slope_x[:, pl.ds(at, chunk)] = jnp.dot(own_smooth, stacked(rise), preferred_element_type=jnp.float32)
        slope_y[:, pl.ds(at, chunk)] = jnp.dot(own_slope, stacked(level), preferred_element_type=jnp.float32)
        return carry

    lax.fori_loop(0, chunks, own_rows, 0, unroll=2)

    @pl.when(me > 0)
    def _():
        down.wait_recv()

    @pl.when(me < n - 1)
    def _():
        up.wait_recv()

    halo_smooth, halo_slope = row_weights(SMOOTH, height, True), row_weights(SLOPE, height, True)

    def halo_rows(i, carry):
        at = pl.multiple_of(i * chunk, chunk)
        rise, level = columns(cells[pl.ds(0, 8), pl.ds(at, chunk + 2 * PAD)])
        slope_x[:, pl.ds(at, chunk)] += jnp.dot(halo_smooth, stacked(rise), preferred_element_type=jnp.float32)
        slope_y[:, pl.ds(at, chunk)] += jnp.dot(halo_slope, stacked(level), preferred_element_type=jnp.float32)
        return carry

    lax.fori_loop(0, chunks, halo_rows, 0, unroll=True)

    def take(k, carry):
        copy_to(k).wait_recv()
        got = recv[k]
        return carry[0] + got[0:8], jnp.maximum(carry[1], got[8:10])

    counts, ends = lax.fori_loop(1, n, take, (send[0:8, :], send[8:10, :]))
    ends = jnp.max(ends, axis=1, keepdims=True)
    span = ends[0:1] + ends[1:2]
    scale = jnp.broadcast_to(zfactor / (8.0 * span) * (1.0 / 4096.0), (8, LANES))

    whole = counts.astype(jnp.int32)
    lane_in = lax.broadcasted_iota(jnp.int32, (LANES, LANES), 0)
    lane_out = lax.broadcasted_iota(jnp.int32, (LANES, LANES), 1)
    triangle = jnp.where(lane_in <= lane_out, 1.0, 0.0).astype(jnp.bfloat16)
    digits = jnp.concatenate([(whole & 255), ((whole >> 8) & 255), (whole >> 16), jnp.zeros_like(whole)],
                             axis=0).astype(jnp.float32).astype(jnp.bfloat16)
    sums = jnp.dot(digits, triangle, preferred_element_type=jnp.float32)
    within = sums[0:8] + 256.0 * sums[8:16] + 65536.0 * sums[16:24]
    before = jnp.zeros((1, 1), jnp.float32)
    rows = []
    rank_load.wait()
    first, second = ranks[0], ranks[1]
    for b in range(8):
        rows.append(before)
        before = before + within[b : b + 1, LANES - 1 : LANES]
    offsets = jnp.concatenate(rows, axis=0)
    cumulative = (within + offsets).astype(jnp.int32)
    divisor = jnp.full((8, LANES), second - first, jnp.int32).astype(jnp.float32)
    table = jnp.clip((cumulative - first).astype(jnp.float32) / divisor, 0.0, 1.0)
    table = table.astype(jnp.bfloat16).astype(jnp.float32)
    out_ref[0:8, :] = table
    out_ref[8:16, :] = scale

    @pl.when(me < n - 1)
    def _():
        down.wait_send()

    @pl.when(me > 0)
    def _():
        up.wait_send()

    def drain(k, carry):
        copy_to(k).wait_send()
        return carry

    lax.fori_loop(1, n, drain, 0)


def shade_kernel(chunk, sums_ref, index_ref, slope_x, slope_y, out_ref, result, out_sem):
    height, width = index_ref.shape
    chunks = width // chunk
    table = sums_ref[0:8, :]
    scale = sums_ref[8:16, :]
    tables = [jnp.broadcast_to(table[b : b + 1], (8, LANES)) for b in range(8)]

    def out_copy(i):
        at = pl.multiple_of(i * chunk, chunk)
        where = (slice(None), pl.ds(at, chunk))
        return pltpu.make_async_copy(result.at[where], out_ref.at[where], out_sem.at[i])

    def finish(i, carry):
        at = pl.multiple_of(i * chunk, chunk)
        for r in range(height // 8):
            for c in range(chunk // LANES):
                rows = pl.ds(8 * r, 8)
                cols = pl.ds(at + c * LANES, LANES)
                which = index_ref[rows, cols]
                group, lane = which >> 7, which & 127
                stretch = jnp.take_along_axis(tables[0], lane, axis=1)
                for b in range(1, 8):
                    stretch = jnp.where(group == b, jnp.take_along_axis(tables[b], lane, axis=1), stretch)
                gx = slope_x[rows, cols] * scale
                gy = slope_y[rows, cols] * scale
                light = (cos_zenith - sin_zenith * (light_x * gx + light_y * gy)) * lax.rsqrt(
                    1.0 + gx * gx + gy * gy)
                result[rows, cols] = stretch * (0.5 + jnp.maximum(light, 0.0))
        out_copy(i).start()
        return carry

    lax.fori_loop(0, chunks, finish, 0)

    def flush(i, carry):
        out_copy(i).wait()
        return carry

    lax.fori_loop(0, chunks, flush, 0)


def chunk_of(width):
    chunk = 1024
    while width % chunk:
        chunk //= 2
    return chunk


def solution(mesh):
    n = mesh.shape["row"]

    def body(elevation, bin_index, ranks):
        height, width = elevation.shape
        chunk = chunk_of(width)
        chunks = width // chunk
        grid = (height, width)
        room = 32 * height * width * 4
        block = pltpu.VMEM(grid, jnp.float32)
        whole = jax.ShapeDtypeStruct(grid, jnp.float32)
        anywhere = pl.BlockSpec(memory_space=pl.ANY)
        inside = pl.BlockSpec(memory_space=pltpu.VMEM)
        sums, index, slope_x, slope_y = pl.pallas_call(
            functools.partial(kernel, n, chunk),
            out_shape=[jax.ShapeDtypeStruct((16, LANES), jnp.float32), jax.ShapeDtypeStruct(grid, jnp.int32), whole, whole],
            in_specs=[anywhere, pl.BlockSpec(memory_space=pltpu.HBM)],
            out_specs=[inside] * 4,
            scratch_shapes=[
                pltpu.VMEM((height + 8, width + 2 * PAD), jnp.float32),
                block,
                block,
                pltpu.VMEM((10, LANES), jnp.float32),
                pltpu.VMEM((n, 10, LANES), jnp.float32),
                pltpu.SMEM((2,), jnp.int32),
                pltpu.SemaphoreType.DMA,
                pltpu.SemaphoreType.DMA,
                pltpu.SemaphoreType.DMA((2,)),
                pltpu.SemaphoreType.DMA((2,)),
                pltpu.SemaphoreType.DMA((n,)),
                pltpu.SemaphoreType.DMA((n,)),
            ],
            compiler_params=pltpu.CompilerParams(collective_id=0, has_side_effects=True, vmem_limit_bytes=room),
        )(ranks, elevation)
        return pl.pallas_call(
            functools.partial(shade_kernel, chunk),
            out_shape=whole,
            in_specs=[inside] * 4,
            out_specs=anywhere,
            scratch_shapes=[block, pltpu.SemaphoreType.DMA((chunks,))],
            compiler_params=pltpu.CompilerParams(vmem_limit_bytes=room),
        )(sums, index, slope_x, slope_y)

    in_specs = (P(("groups", "row"), None), P(("groups", "row"), None), P("groups"))
    return jax.shard_map(body, mesh=mesh, in_specs=in_specs, out_specs=P(("groups", "row"), None), check_vma=False)
```
